256 devices in a mesh: ta: 16 (over z, core), gy: 2 (over x_lo), gx: 8 (over x_hi, y).
Axes of the slice: x: 4 (x_hi: 2, x_lo: 2; x = x_hi * 2 + x_lo), y: 4, z: 8, core: 2. Of those that a mesh axis runs over, the one named last changes fastest.
Arguments:
- queries: bfloat16 [16, 2, 16, 64, 1536], P('ta', 'gy', 'gx'), may hold values from -24 to 24
- keys: bfloat16 [16, 2, 16, 64, 1536], P('ta', 'gy', 'gx'), may hold values from -24 to 24
- values: bfloat16 [16, 2, 16, 64, 1536], P('ta', 'gy', 'gx'), may hold values from -6 to 6
- grad_out: bfloat16 [16, 2, 16, 64, 1536], P('ta', 'gy', 'gx'), may hold values from -6 to 6
Outputs:
- attention: bfloat16 [16, 2, 16, 64, 1536], P('ta', 'gy', 'gx')
- grad_queries: bfloat16 [16, 2, 16, 64, 1536], P('ta', 'gy', 'gx')
- grad_keys: bfloat16 [16, 2, 16, 64, 1536], P('ta', 'gy', 'gx')
- grad_values: bfloat16 [16, 2, 16, 64, 1536], P('ta', 'gy', 'gx')
The draws below stay inside these ranges and needn't reach their ends.
All inputs are finite; a program needn't handle non-finite values.
Results may differ from the reference program's by a relative error of at most 0.019.
Values may be sent and summed in bfloat16 or wider, within the bound.
A program may use at most 128 MiB of HBM per device.

```python
import jax
import jax.numpy as jnp
from jax import lax

HEADS = 12
HEAD_DIM = 128
TILE = 8
FRAMES = 16
TROWS = 2
TCOLS = 16


def joint_tiles(key):
    extent = (FRAMES, TROWS, TCOLS, TILE * TILE, HEADS * HEAD_DIM)
    query_base = jnp.clip(jax.random.normal(jax.random.fold_in(key, 11), extent, jnp.float32), -6.0, 6.0)
    key_base = jnp.clip(jax.random.normal(jax.random.fold_in(key, 12), extent, jnp.float32), -6.0, 6.0)
    return (jnp.clip(query_base, -24.0, 24.0), jnp.clip(key_base, -24.0, 24.0))


def draw_queries(key, part):
    return joint_tiles(key)[0].astype(jnp.bfloat16)


def draw_keys(key, part):
    return joint_tiles(key)[1].astype(jnp.bfloat16)


def block_levels(key, shape, shards, least, top_value):
    factor_of, own = 1.0, jax.random.fold_in(key, 6)
    for position, shards_of in shards:
        heights = jnp.exp(jax.random.uniform(jax.random.fold_in(own, position), (shards_of,), jnp.float32, least / len(shards), top_value / len(shards)))
        factor_of = factor_of * jnp.repeat(heights, shape[position] // shards_of).reshape([-1 if axis == position else 1 for axis in range(len(shape))])
    return factor_of


def normal_values(stream_key, shape, spread, most, cuts=(), kind=jnp.bfloat16):
    factor_of = block_levels(stream_key, shape, cuts, -0.22, 0.18) if cuts else 1.0
    values = jax.random.normal(stream_key, shape, jnp.float32) * spread * factor_of
    return jnp.minimum(jnp.maximum(values, -most), most).astype(kind)


def setup_inputs(seed: int = 0) -> dict:
    key_of = jax.random.split(jax.random.key(seed), 5)
    queries = draw_queries(jax.random.fold_in(key_of[4], 71), 0)
    keys = draw_keys(jax.random.fold_in(key_of[4], 71), 0)
    values = normal_values(key_of[2], (FRAMES, TROWS, TCOLS, TILE * TILE, HEADS * HEAD_DIM), 1.0, 6.0, ((0, 16), (1, 2), (2, 8)))
    grad_out = normal_values(key_of[3], (FRAMES, TROWS, TCOLS, TILE * TILE, HEADS * HEAD_DIM), 1.0, 6.0, ((0, 16), (1, 2), (2, 8)))
    return dict(queries=queries, keys=keys, values=values, grad_out=grad_out)


def windows(padded, frame_index):
    frame_slab = lax.dynamic_slice_in_dim(padded, frame_index, 3, 0)
    pieces = [frame_slab[frame_step, row_step:row_step + TROWS, col_step:col_step + TCOLS]
              for frame_step in range(3) for row_step in range(3) for col_step in range(3)]
    return jnp.stack(pieces, axis=2)


def pad_tiles(array):
    return jnp.pad(array, ((1, 1), (1, 1), (1, 1)) + ((0, 0),) * (array.ndim - 3))


def rounded(array):
    return lax.optimization_barrier(array.astype(jnp.bfloat16)).astype(jnp.float32)


def reference(queries, keys, values, grad_out):
    tokens = TILE * TILE
    near_tokens = 27 * tokens
    factor = HEAD_DIM ** -0.5
    inside = pad_tiles(jnp.ones((FRAMES, TROWS, TCOLS), jnp.float32))
    near_extent = (TROWS, TCOLS, near_tokens, HEADS, HEAD_DIM)
    own_extent = (TROWS, TCOLS, tokens, HEADS, HEAD_DIM)
    flat_extent = (TROWS, TCOLS, tokens, HEADS * HEAD_DIM)
    key_pad = pad_tiles(keys)
    value_pad = pad_tiles(values)

    def allowed_at(frame_index):
        return (jnp.repeat(windows(inside, frame_index), tokens, axis=2) > 0.5)[:, :, None, None, :]

    def own_tiles(array, frame_index):
        return lax.dynamic_index_in_dim(array, frame_index, 0, False).astype(jnp.float32).reshape(own_extent)

    def query_pass(frame_index):
        query_here = own_tiles(queries, frame_index)
        grad_here = own_tiles(grad_out, frame_index)
        key_near = windows(key_pad, frame_index).astype(jnp.float32).reshape(near_extent)
        value_near = windows(value_pad, frame_index).astype(jnp.float32).reshape(near_extent)
        allowed = allowed_at(frame_index)
        scores = jnp.einsum("rcihd,rcjhd->rchij", query_here, key_near) * factor
        scores = jnp.where(allowed, scores, -jnp.inf)
        highest = jnp.max(scores, axis=4, keepdims=True)
        log_total = highest + jnp.log(jnp.sum(jnp.exp(scores - highest), axis=4, keepdims=True))
        weights = jnp.exp(scores - log_total)
        attended = jnp.einsum("rchij,rcjhd->rcihd", rounded(weights), value_near).astype(jnp.bfloat16)
        row_dots = jnp.sum(grad_here * lax.optimization_barrier(attended).astype(jnp.float32), axis=4)
        row_dots = jnp.transpose(row_dots, (0, 1, 3, 2))
        pulls = jnp.einsum("rcihd,rcjhd->rchij", grad_here, value_near)
        slopes = weights * (pulls - row_dots[:, :, :, :, None])
        grad_query = (jnp.einsum("rchij,rcjhd->rcihd", rounded(slopes), key_near) * factor).astype(jnp.bfloat16)
        return (attended.reshape(flat_extent), grad_query.reshape(flat_extent), log_total[:, :, :, :, 0], row_dots)

    frame_list = jnp.arange(FRAMES, dtype=jnp.int32)
    attention, grad_queries, totals, dots_all = lax.map(query_pass, frame_list)
    query_pad = pad_tiles(queries)
    grad_pad = pad_tiles(grad_out)
    total_pad = pad_tiles(totals)
    dots_pad = pad_tiles(dots_all)

    def stat_near(padded, frame_index):
        picked = jnp.transpose(windows(padded, frame_index), (0, 1, 3, 2, 4))
        return picked.reshape(TROWS, TCOLS, HEADS, near_tokens)

    def key_pass(frame_index):
        key_here = own_tiles(keys, frame_index)
        value_here = own_tiles(values, frame_index)
        query_near = windows(query_pad, frame_index).astype(jnp.float32).reshape(near_extent)
        grad_near = windows(grad_pad, frame_index).astype(jnp.float32).reshape(near_extent)
        total_near = stat_near(total_pad, frame_index)
        dots_near = stat_near(dots_pad, frame_index)
        allowed = allowed_at(frame_index)
        scores = jnp.einsum("rcihd,rcjhd->rchij", key_here, query_near) * factor
        weights = jnp.exp(jnp.where(allowed, scores - total_near[:, :, :, None, :], -jnp.inf))
        pulls = jnp.einsum("rcihd,rcjhd->rchij", value_here, grad_near)
        slopes = weights * (pulls - dots_near[:, :, :, None, :])
        grad_value = jnp.einsum("rchij,rcjhd->rcihd", rounded(weights), grad_near).astype(jnp.bfloat16)
        grad_key = (jnp.einsum("rchij,rcjhd->rcihd", rounded(slopes), query_near) * factor).astype(jnp.bfloat16)
        return (grad_key.reshape(flat_extent), grad_value.reshape(flat_extent))

    grad_keys, grad_values = lax.map(key_pass, frame_list)
    return (attention, grad_queries, grad_keys, grad_values)
```

```python
import jax
import jax.numpy as jnp
from jax import lax
from jax.experimental import pallas as pl
from jax.experimental.pallas import tpu as pltpu
from jax.sharding import PartitionSpec as P

MESH = pl.DeviceIdType.MESH
DIM = 128
TOK = 64
CHUNKS = 3
FACTOR = DIM ** -0.5
SCALE = FACTOR * 1.4426950408889634
FAR = 1e30
FRAMES = 16
TCOLS = 16
NT = (((1,), (1,)), ((), ()))
NN = (((1,), (0,)), ((), ()))


def dot_nt(a, b):
    return lax.dot_general(a, b, NT, preferred_element_type=jnp.float32)


def dot_nn(a, b):
    return lax.dot_general(a, b, NN, preferred_element_type=jnp.float32)


def kernel(
    q_in, k_in, v_in, g_in, out_o, out_dq, out_dk, out_dv,
    kv, qg, st, stage,
    local_sem, in_send, in_recv, y_send, y_recv, z_send, z_recv,
    sy_send, sy_recv, sz_send, sz_recv, keep_sem, back_send, back_recv,
):
    ta = lax.axis_index("ta")
    xl = lax.axis_index("gy")
    gx = lax.axis_index("gx")
    z, core = ta // 2, ta % 2
    xh = gx // 4
    side = (xl + xh) % 2

    def along_y(step):
        other = (gx + step + 8) % 8
        return (ta, (side + other // 4) % 2, other)

    def along_z(step):
        return (((z + step + 8) % 8) * 2 + core, xl, gx)

    peers = ((0, 1), (1, 0), (1, 1))

    def peer_id(p):
        dx, dc = peers[p]
        return (z * 2 + (core + dc) % 2, (xl + dx) % 2, gx)

    def peer_group(p):
        dx, dc = peers[p]
        return 2 * ((side + dx) % 2) + (core + dc) % 2

    my_group = 2 * side + core
    y_ids = (along_y(1), along_y(-1))
    z_ids = (along_z(1), along_z(-1))

    barrier = pltpu.get_barrier_semaphore()
    for target in (peer_id(0), peer_id(1), peer_id(2), *y_ids, *z_ids):
        pl.semaphore_signal(barrier, inc=1, device_id=target, device_id_type=MESH)
    pl.semaphore_wait(barrier, 7)

    def lanes(group, j):
        return pl.ds(pl.multiple_of((group * CHUNKS + j) * DIM, DIM), DIM)

    sources = (k_in, v_in, q_in, g_in)
    results = (out_o, out_dq, out_dk, out_dv)

    def slot(t, j):
        held = kv if t < 2 else qg
        return held.at[j, t % 2, pl.ds(1, 2), 1 + core, xl]

    def local_copy(j, t):
        return pltpu.make_async_copy(
            sources[t].at[0, 0, :, :, lanes(my_group, j)], slot(t, j), local_sem.at[j, t]
        )

    def in_copy(p, j, t):
        return pltpu.make_async_remote_copy(
            src_ref=sources[t].at[0, 0, :, :, lanes(peer_group(p), j)],
            dst_ref=slot(t, j),
            send_sem=in_send.at[p, j, t],
            recv_sem=in_recv.at[p, j, t],
            device_id=peer_id(p),
            device_id_type=MESH,
        )

    def remote(src, dst, send, recv, target):
        return pltpu.make_async_remote_copy(
            src_ref=src, dst_ref=dst, send_sem=send, recv_sem=recv,
            device_id=target, device_id_type=MESH,
        )

    def kv_y(j, w, d):
        row = (xl + w) % 2
        return remote(
            kv.at[j, :, 2 - d, pl.ds(1, 2), row], kv.at[j, :, 3 * d, pl.ds(1, 2), row],
            y_send.at[0, j, w, d], y_recv.at[0, j, row, d], y_ids[d],
        )

    def qg_z(j, w, d):
        row = (xl + w) % 2
        return remote(
            qg.at[j, :, pl.ds(1, 2), 2 - d, row], qg.at[j, :, pl.ds(1, 2), 3 * d, row],
            z_send.at[0, j, w, d], z_recv.at[0, j, row, d], z_ids[d],
        )

    def kv_z(j, d):
        return remote(
            kv.at[j, :, :, 2 - d], kv.at[j, :, :, 3 * d],
            z_send.at[1, j, 0, d], z_recv.at[1, j, 0, d], z_ids[d],
        )

    def qg_y(j, d):
        return remote(
            qg.at[j, :, 2 - d], qg.at[j, :, 3 * d],
            y_send.at[1, j, 0, d], y_recv.at[1, j, 0, d], y_ids[d],
        )

    def st_y(j, d):
        return remote(
            st.at[j, 2 - d, pl.ds(1, 2)], st.at[j, 3 * d, pl.ds(1, 2)],
            sy_send.at[j, d], sy_recv.at[j, d], y_ids[d],
        )

    def st_z(j, d):
        return remote(
            st.at[j, :, 2 - d], st.at[j, :, 3 * d],
            sz_send.at[j, d], sz_recv.at[j, d], z_ids[d],
        )

    def keep_copy(t, j):
        return pltpu.make_async_copy(
            stage.at[t, j, :, core, xl], results[t].at[0, 0, :, :, lanes(my_group, j)],
            keep_sem.at[t, j],
        )

    def back_copy(p, t, j):
        dx, dc = peers[p]
        return remote(
            stage.at[t, j, :, (core + dc) % 2, (xl + dx) % 2],
            results[t].at[0, 0, :, :, lanes(my_group, j)],
            back_send.at[p, t, j], back_recv.at[p, t, j], peer_id(p),
        )

    for j in range(CHUNKS):
        for t in range(4):
            local_copy(j, t).start()
            in_copy(0, j, t).start()
    for j in range(CHUNKS):
        for t in range(4):
            for p in (1, 2):
                in_copy(p, j, t).start()

    def first_hops(j, w):
        for half in range(2):
            for t in (2 * half, 2 * half + 1):
                if w == 0:
                    local_copy(j, t).wait()
                    in_copy(0, j, t).wait_recv()
                else:
                    in_copy(1, j, t).wait_recv()
                    in_copy(2, j, t).wait_recv()
            for d in range(2):
                (kv_y if half == 0 else qg_z)(j, w, d).start()

    def second_hops(j):
        for d in range(2):
            kv_y(j, 0, d).wait_recv()
            kv_y(j, 1, d).wait_recv()
        for d in range(2):
            kv_z(j, d).start()
        for d in range(2):
            qg_z(j, 0, d).wait_recv()
            qg_z(j, 1, d).wait_recv()
        for d in range(2):
            qg_y(j, d).start()

    def in_grid(c, f, dc, df):
        col = 2 * gx + c + dc - 1
        frame = 2 * z + f + df - 1
        return (col >= 0) & (col < TCOLS) & (frame >= 0) & (frame < FRAMES)

    lane = lax.broadcasted_iota(jnp.int32, (DIM, DIM), 1)

    def query_block(j, c, f):
        q = qg[j, 0, 1 + c, 1 + f].reshape(2 * TOK, DIM)
        g = qg[j, 1, 1 + c, 1 + f].reshape(2 * TOK, DIM)
        scores = []
        for dc in range(3):
            s = dot_nt(q, kv[j, 0, c + dc, pl.ds(f, 3)].reshape(6 * TOK, DIM))
            parts = [
                s[:, df * DIM:(df + 1) * DIM] * SCALE
                + jnp.where(in_grid(c, f, dc, df), 0.0, -FAR)
                for df in range(3)
            ]
            scores.append(jnp.concatenate(parts, axis=1))
        top = jnp.maximum(jnp.maximum(scores[0], scores[1]), scores[2])
        top = jnp.max(top, axis=1, keepdims=True)
        powers = [jnp.exp2(s - top) for s in scores]
        total = jnp.sum(powers[0] + powers[1] + powers[2], axis=1, keepdims=True)
        scale = 1.0 / total
        att = jnp.zeros((2 * TOK, DIM), jnp.float32)
        for dc in range(3):
            v = kv[j, 1, c + dc, pl.ds(f, 3)].reshape(6 * TOK, DIM)
            att += dot_nn(powers[dc].astype(jnp.bfloat16), v)
        att = (att * scale).astype(jnp.bfloat16)
        dots = jnp.sum(g.astype(jnp.float32) * att.astype(jnp.float32), axis=1, keepdims=True)
        grad = jnp.zeros((2 * TOK, DIM), jnp.float32)
        for dc in range(3):
            k = kv[j, 0, c + dc, pl.ds(f, 3)].reshape(6 * TOK, DIM)
            v = kv[j, 1, c + dc, pl.ds(f, 3)].reshape(6 * TOK, DIM)
            slopes = powers[dc] * (dot_nt(g, v) - dots)
            grad += dot_nn(slopes.astype(jnp.bfloat16), k)
        grad = (grad * (scale * FACTOR)).astype(jnp.bfloat16)
        stage[0, j, c, f] = att.reshape(2, TOK, DIM)
        stage[1, j, c, f] = grad.reshape(2, TOK, DIM)
        both = jnp.where(lane == 0, top + jnp.log2(total), dots)
        st[j, 1 + c, 1 + f] = jnp.transpose(both)[:8]

    def key_block(j, c, f):
        k = kv[j, 0, 1 + c, 1 + f].reshape(2 * TOK, DIM)
        v = kv[j, 1, 1 + c, 1 + f].reshape(2 * TOK, DIM)
        grad_k = jnp.zeros((2 * TOK, DIM), jnp.float32)
        grad_v = jnp.zeros((2 * TOK, DIM), jnp.float32)
        for dc in range(3):
            q = qg[j, 0, c + dc, pl.ds(f, 3)].reshape(6 * TOK, DIM)
            g = qg[j, 1, c + dc, pl.ds(f, 3)].reshape(6 * TOK, DIM)
            s = dot_nt(k, q)
            pulls = dot_nt(v, g)
            weights, slopes = [], []
            for df in range(3):
                tile = st[j, c + dc, f + df]
                level = jnp.where(in_grid(c, f, dc, df), tile[0:1], FAR)
                cut = slice(df * DIM, (df + 1) * DIM)
                w = jnp.exp2(s[:, cut] * SCALE - level)
                weights.append(w.astype(jnp.bfloat16))
                slopes.append((w * (pulls[:, cut] - tile[1:2])).astype(jnp.bfloat16))
            grad_v += dot_nn(jnp.concatenate(weights, axis=1), g)
            grad_k += dot_nn(jnp.concatenate(slopes, axis=1), q)
        stage[2, j, c, f] = (grad_k * FACTOR).astype(jnp.bfloat16).reshape(2, TOK, DIM)
        stage[3, j, c, f] = grad_v.astype(jnp.bfloat16).reshape(2, TOK, DIM)

    def blocks(run, j, first, last):
        def one(i, carry):
            run(j, i // 2, i % 2)
            return carry

        lax.fori_loop(first, last, one, 0)

    def send_back(j, ts):
        for t in ts:
            for p in (1, 2, 0):
                back_copy(p, t, j).start()
            keep_copy(t, j).start()

    def query_side(j):
        for d in range(2):
            kv_z(j, d).wait_recv()
        blocks(query_block, j, 0, 4)
        for d in range(2):
            st_y(j, d).start()
        send_back(j, (0, 1))

    def pass_stats(j):
        for d in range(2):
            st_y(j, d).wait_recv()
        for d in range(2):
            st_z(j, d).start()

    def key_ready(j):
        for d in range(2):
            qg_y(j, d).wait_recv()
        for d in range(2):
            st_z(j, d).wait_recv()

    for j in range(CHUNKS):
        first_hops(j, 0)
    first_hops(0, 1)
    second_hops(0)
    first_hops(1, 1)
    second_hops(1)
    first_hops(2, 1)
    query_side(0)
    second_hops(2)
    pass_stats(0)
    query_side(1)
    key_ready(0)
    blocks(key_block, 0, 0, 4)
    send_back(0, (2, 3))
    pass_stats(1)
    query_side(2)
    key_ready(1)
    blocks(key_block, 1, 0, 2)
    pass_stats(2)
    blocks(key_block, 1, 2, 4)
    send_back(1, (2, 3))
    key_ready(2)
    blocks(key_block, 2, 0, 4)
    send_back(2, (2, 3))

    for j in range(CHUNKS):
        for t in range(4):
            for p in range(3):
                in_copy(p, j, t).wait_send()
        for d in range(2):
            for w in range(2):
                kv_y(j, w, d).wait_send()
                qg_z(j, w, d).wait_send()
            kv_z(j, d).wait_send()
            qg_y(j, d).wait_send()
            st_y(j, d).wait_send()
            st_z(j, d).wait_send()
        for t in range(4):
            keep_copy(t, j).wait()
            for p in range(3):
                back_copy(p, t, j).wait_send()
                back_copy(p, t, j).wait_recv()


def body(queries, keys, values, grad_out):
    dma = pltpu.SemaphoreType.DMA
    block = (CHUNKS, 2, 4, 4, 2, TOK, DIM)
    return pl.pallas_call(
        kernel,
        out_shape=[jax.ShapeDtypeStruct(queries.shape, jnp.bfloat16)] * 4,
        in_specs=[pl.BlockSpec(memory_space=pl.ANY)] * 4,
        out_specs=[pl.BlockSpec(memory_space=pl.ANY)] * 4,
        scratch_shapes=[
            pltpu.VMEM(block, jnp.bfloat16),
            pltpu.VMEM(block, jnp.bfloat16),
            pltpu.VMEM((CHUNKS, 4, 4, 8, DIM), jnp.float32),
            pltpu.VMEM((4, CHUNKS, 2, 2, 2, TOK, DIM), jnp.bfloat16),
            dma((CHUNKS, 4)),
            dma((3, CHUNKS, 4)),
            dma((3, CHUNKS, 4)),
            dma((2, CHUNKS, 2, 2)),
            dma((2, CHUNKS, 2, 2)),
            dma((2, CHUNKS, 2, 2)),
            dma((2, CHUNKS, 2, 2)),
            dma((CHUNKS, 2)),
            dma((CHUNKS, 2)),
            dma((CHUNKS, 2)),
            dma((CHUNKS, 2)),
            dma((4, CHUNKS)),
            dma((3, 4, CHUNKS)),
            dma((3, 4, CHUNKS)),
        ],
        compiler_params=pltpu.CompilerParams(
            collective_id=0, has_side_effects=True, vmem_limit_bytes=48 * 1024 * 1024
        ),
    )(queries, keys, values, grad_out)


def solution(mesh):
    spec = P("ta", "gy", "gx", None, None)
    return jax.shard_map(
        body, mesh=mesh, in_specs=(spec,) * 4, out_specs=(spec,) * 4, check_vma=False
    )
```

```python
import jax
import jax.numpy as jnp
from jax import lax
from jax.experimental import pallas as pl
from jax.experimental.pallas import tpu as pltpu
from jax.sharding import PartitionSpec as P

MESH = pl.DeviceIdType.MESH
DIM = 128
TOK = 64
CHUNKS = 3
FACTOR = DIM ** -0.5
SCALE = FACTOR * 1.4426950408889634
FAR = 1e30
FRAMES = 16
TCOLS = 16
NT = (((1,), (1,)), ((), ()))
NN = (((1,), (0,)), ((), ()))


def dot_nt(a, b):
    return lax.dot_general(a, b, NT, preferred_element_type=jnp.float32)


def dot_nn(a, b):
    return lax.dot_general(a, b, NN, preferred_element_type=jnp.float32)


def kernel(
    q_in, k_in, v_in, g_in, out_o, out_dq, out_dk, out_dv,
    kv, qg, st, stage,
    local_sem, in_send, in_recv, y_send, y_recv, z_send, z_recv,
    cy_send, cy_recv, cz_send, cz_recv, st_send, st_recv, keep_sem, back_send, back_recv,
):
    ta = lax.axis_index("ta")
    xl = lax.axis_index("gy")
    gx = lax.axis_index("gx")
    z, core = ta // 2, ta % 2
    xh = gx // 4
    side = (xl + xh) % 2

    def along_y(step):
        other = (gx + step + 8) % 8
        return (ta, (side + other // 4) % 2, other)

    def along_z(step):
        return (((z + step + 8) % 8) * 2 + core, xl, gx)

    peers = ((0, 1), (1, 0), (1, 1))

    def peer_id(p):
        dx, dc = peers[p]
        return (z * 2 + (core + dc) % 2, (xl + dx) % 2, gx)

    def peer_group(p):
        dx, dc = peers[p]
        return 2 * ((side + dx) % 2) + (core + dc) % 2

    my_group = 2 * side + core
    around = ((1, 0), (-1, 0), (0, 1), (0, -1), (1, 1), (1, -1), (-1, 1), (-1, -1))
    around_ids = tuple((along_z(dz)[0], *along_y(dy)[1:]) for dy, dz in around)
    y_ids, z_ids = around_ids[:2], around_ids[2:4]

    barrier = pltpu.get_barrier_semaphore()
    for target in (peer_id(0), peer_id(1), peer_id(2), *around_ids):
        pl.semaphore_signal(barrier, inc=1, device_id=target, device_id_type=MESH)
    pl.semaphore_wait(barrier, 11)

    def lanes(group, j):
        return pl.ds(pl.multiple_of((group * CHUNKS + j) * DIM, DIM), DIM)

    sources = (k_in, v_in, q_in, g_in)
    results = (out_o, out_dq, out_dk, out_dv)

    def slot(t, j):
        held = kv if t < 2 else qg
        return held.at[j, t % 2, pl.ds(1, 2), 1 + core, xl]

    def local_copy(j, t):
        return pltpu.make_async_copy(
            sources[t].at[0, 0, :, :, lanes(my_group, j)], slot(t, j), local_sem.at[j, t]
        )

    def in_copy(p, j, t):
        return pltpu.make_async_remote_copy(
            src_ref=sources[t].at[0, 0, :, :, lanes(peer_group(p), j)],
            dst_ref=slot(t, j),
            send_sem=in_send.at[p, j, t],
            recv_sem=in_recv.at[p, j, t],
            device_id=peer_id(p),
            device_id_type=MESH,
        )

    def remote(src, dst, send, recv, target):
        return pltpu.make_async_remote_copy(
            src_ref=src, dst_ref=dst, send_sem=send, recv_sem=recv,
            device_id=target, device_id_type=MESH,
        )

    def edge_y(h, j, w, d):
        row = (xl + w) % 2
        held = (kv, qg)[h]
        return remote(
            held.at[j, :, 2 - d, pl.ds(1, 2), row], held.at[j, :, 3 * d, pl.ds(1, 2), row],
            y_send.at[h, j, w, d], y_recv.at[h, j, row, d], y_ids[d],
        )

    def edge_z(h, j, w, d):
        row = (xl + w) % 2
        held = (kv, qg)[h]
        return remote(
            held.at[j, :, pl.ds(1, 2), 2 - d, row], held.at[j, :, pl.ds(1, 2), 3 * d, row],
            z_send.at[h, j, w, d], z_recv.at[h, j, row, d], z_ids[d],
        )

    def corner_z(j, e, d):
        return remote(
            kv.at[j, :, 3 * e, 2 - d], kv.at[j, :, 3 * e, 3 * d],
            cz_send.at[j, e, d], cz_recv.at[j, e, d], z_ids[d],
        )

    def corner_y(j, e, d):
        return remote(
            qg.at[j, :, 2 - d, 3 * e], qg.at[j, :, 3 * d, 3 * e],
            cy_send.at[j, e, d], cy_recv.at[j, e, d], y_ids[d],
        )

    def stat_copy(j, n):
        dy, dz = around[n]
        cols = {0: (pl.ds(1, 2), pl.ds(1, 2)), 1: (2, 0), -1: (1, 3)}[dy]
        frames = {0: (pl.ds(1, 2), pl.ds(1, 2)), 1: (2, 0), -1: (1, 3)}[dz]
        return remote(
            st.at[j, cols[0], frames[0]], st.at[j, cols[1], frames[1]],
            st_send.at[j, n], st_recv.at[j, n], around_ids[n],
        )

    def keep_copy(t, j):
        return pltpu.make_async_copy(
            stage.at[t, j, :, core, xl], results[t].at[0, 0, :, :, lanes(my_group, j)],
            keep_sem.at[t, j],
        )

    def back_copy(p, t, j):
        dx, dc = peers[p]
        return remote(
            stage.at[t, j, :, (core + dc) % 2, (xl + dx) % 2],
            results[t].at[0, 0, :, :, lanes(my_group, j)],
            back_send.at[p, t, j], back_recv.at[p, t, j], peer_id(p),
        )

    for j in range(CHUNKS):
        for t in range(4):
            local_copy(j, t).start()
            in_copy(0, j, t).start()
    for j in range(CHUNKS):
        for t in range(4):
            for p in (1, 2):
                in_copy(p, j, t).start()

    def first_hops(j, w):
        for h in range(2):
            for t in (2 * h, 2 * h + 1):
                if w == 0:
                    local_copy(j, t).wait()
                    in_copy(0, j, t).wait_recv()
                else:
                    in_copy(1, j, t).wait_recv()
                    in_copy(2, j, t).wait_recv()
            for d in range(2):
                edge_y(h, j, w, d).start()
                edge_z(h, j, w, d).start()

    def second_hops(j):
        for d in range(2):
            for w in range(2):
                edge_y(0, j, w, d).wait_recv()
        for e in range(2):
            for d in range(2):
                corner_z(j, e, d).start()
        for d in range(2):
            for w in range(2):
                edge_z(1, j, w, d).wait_recv()
        for e in range(2):
            for d in range(2):
                corner_y(j, e, d).start()

    def in_grid(c, f, dc, df):
        col = 2 * gx + c + dc - 1
        frame = 2 * z + f + df - 1
        return (col >= 0) & (col < TCOLS) & (frame >= 0) & (frame < FRAMES)

    lane = lax.broadcasted_iota(jnp.int32, (DIM, DIM), 1)

    def pair(half0, half1):
        blank = jnp.zeros((2 * TOK, DIM), half0.dtype)
        return jnp.concatenate(
            [jnp.concatenate([half0, blank], axis=1), jnp.concatenate([blank, half1], axis=1)],
            axis=0,
        )

    def halves(x):
        return x[:2 * TOK, :3 * DIM], x[2 * TOK:, DIM:]

    def query_block(j, c):
        q = qg[j, 0, 1 + c, 1:3].reshape(4 * TOK, DIM)
        g = qg[j, 1, 1 + c, 1:3].reshape(4 * TOK, DIM)
        scores = [[], []]
        for dc in range(3):
            s = dot_nt(q, kv[j, 0, c + dc].reshape(8 * TOK, DIM))
            for f, part in enumerate(halves(s)):
                scores[f].append(jnp.concatenate([
                    part[:, df * DIM:(df + 1) * DIM] * SCALE
                    + jnp.where(in_grid(c, f, dc, df), 0.0, -FAR)
                    for df in range(3)
                ], axis=1))
        tops, powers, totals = [], [], []
        for f in range(2):
            top = jnp.maximum(jnp.maximum(scores[f][0], scores[f][1]), scores[f][2])
            top = jnp.max(top, axis=1, keepdims=True)
            p = [jnp.exp2(s - top) for s in scores[f]]
            tops.append(top)
            powers.append(p)
            totals.append(jnp.sum(p[0] + p[1] + p[2], axis=1, keepdims=True))
        top = jnp.concatenate(tops, axis=0)
        total = jnp.concatenate(totals, axis=0)
        scale = 1.0 / total
        att = jnp.zeros((4 * TOK, DIM), jnp.float32)
        for dc in range(3):
            v = kv[j, 1, c + dc].reshape(8 * TOK, DIM)
            att += dot_nn(pair(*(powers[f][dc].astype(jnp.bfloat16) for f in range(2))), v)
        att = (att * scale).astype(jnp.bfloat16)
        dots = jnp.sum(g.astype(jnp.float32) * att.astype(jnp.float32), axis=1, keepdims=True)
        grad = jnp.zeros((4 * TOK, DIM), jnp.float32)
        for dc in range(3):
            k = kv[j, 0, c + dc].reshape(8 * TOK, DIM)
            v = kv[j, 1, c + dc].reshape(8 * TOK, DIM)
            pulls = halves(dot_nt(g, v))
            slopes = (
                (powers[f][dc] * (pulls[f] - dots[f * 2 * TOK:(f + 1) * 2 * TOK])).astype(jnp.bfloat16)
                for f in range(2)
            )
            grad += dot_nn(pair(*slopes), k)
        grad = (grad * (scale * FACTOR)).astype(jnp.bfloat16)
        stage[0, j, c] = att.reshape(2, 2, TOK, DIM)
        stage[1, j, c] = grad.reshape(2, 2, TOK, DIM)
        level = top + jnp.log2(total)
        for f in range(2):
            cut = slice(f * 2 * TOK, (f + 1) * 2 * TOK)
            st[j, 1 + c, 1 + f] = jnp.transpose(jnp.where(lane == 0, level[cut], dots[cut]))[:8]

    def key_block(j, c):
        k = kv[j, 0, 1 + c, 1:3].reshape(4 * TOK, DIM)
        v = kv[j, 1, 1 + c, 1:3].reshape(4 * TOK, DIM)
        grad_k = jnp.zeros((4 * TOK, DIM), jnp.float32)
        grad_v = jnp.zeros((4 * TOK, DIM), jnp.float32)
        for dc in range(3):
            q = qg[j, 0, c + dc].reshape(8 * TOK, DIM)
            g = qg[j, 1, c + dc].reshape(8 * TOK, DIM)
            s = halves(dot_nt(k, q))
            pulls = halves(dot_nt(v, g))
            weights, slopes = [], []
            for f in range(2):
                ws, ss = [], []
                for df in range(3):
                    tile = st[j, c + dc, f + df]
                    level = jnp.where(in_grid(c, f, dc, df), tile[0:1], FAR)
                    cut = slice(df * DIM, (df + 1) * DIM)
                    w = jnp.exp2(s[f][:, cut] * SCALE - level)
                    ws.append(w.astype(jnp.bfloat16))
                    ss.append((w * (pulls[f][:, cut] - tile[1:2])).astype(jnp.bfloat16))
                weights.append(jnp.concatenate(ws, axis=1))
                slopes.append(jnp.concatenate(ss, axis=1))
            grad_v += dot_nn(pair(*weights), g)
            grad_k += dot_nn(pair(*slopes), q)
        stage[2, j, c] = (grad_k * FACTOR).astype(jnp.bfloat16).reshape(2, 2, TOK, DIM)
        stage[3, j, c] = grad_v.astype(jnp.bfloat16).reshape(2, 2, TOK, DIM)

    def blocks(run, j):
        def one(c, carry):
            run(j, c)
            return carry

        lax.fori_loop(0, 2, one, 0)

    def send_back(j, ts):
        for t in ts:
            for p in (1, 2, 0):
                back_copy(p, t, j).start()
            keep_copy(t, j).start()

    def query_side(j):
        for d in range(2):
            for w in range(2):
                edge_z(0, j, w, d).wait_recv()
        for e in range(2):
            for d in range(2):
                corner_z(j, e, d).wait_recv()
        blocks(query_block, j)
        for n in range(8):
            stat_copy(j, n).start()
        send_back(j, (0, 1))

    def key_side(j):
        for d in range(2):
            for w in range(2):
                edge_y(1, j, w, d).wait_recv()
        for e in range(2):
            for d in range(2):
                corner_y(j, e, d).wait_recv()
        for n in range(8):
            stat_copy(j, n).wait_recv()
        blocks(key_block, j)
        send_back(j, (2, 3))

    first_hops(0, 0)
    first_hops(1, 0)
    first_hops(0, 1)
    first_hops(2, 0)
    second_hops(0)
    first_hops(1, 1)
    first_hops(2, 1)
    second_hops(1)
    query_side(0)
    second_hops(2)
    query_side(1)
    key_side(0)
    query_side(2)
    key_side(1)
    key_side(2)
    for j in range(CHUNKS):
        for t in range(4):
            for p in range(3):
                in_copy(p, j, t).wait_send()
        for d in range(2):
            for w in range(2):
                for h in range(2):
                    edge_y(h, j, w, d).wait_send()
                    edge_z(h, j, w, d).wait_send()
            for e in range(2):
                corner_z(j, e, d).wait_send()
                corner_y(j, e, d).wait_send()
        for n in range(8):
            stat_copy(j, n).wait_send()
        for t in range(4):
            keep_copy(t, j).wait()
            for p in range(3):
                back_copy(p, t, j).wait_send()
                back_copy(p, t, j).wait_recv()


def drain(*refs):
    held, out, sem = refs[:4], refs[4:8], refs[8]
    copies = [pltpu.make_async_copy(held[t], out[t], sem.at[t]) for t in range(4)]
    for copy in copies:
        copy.start()
    for copy in copies:
        copy.wait()


def body(queries, keys, values, grad_out):
    dma = pltpu.SemaphoreType.DMA
    block = (CHUNKS, 2, 4, 4, 2, TOK, DIM)
    held = pl.pallas_call(
        kernel,
        out_shape=[jax.ShapeDtypeStruct(queries.shape, jnp.bfloat16)] * 4,
        in_specs=[pl.BlockSpec(memory_space=pl.ANY)] * 4,
        out_specs=[pl.BlockSpec(memory_space=pl.ANY)] * 4,
        scratch_shapes=[
            pltpu.VMEM(block, jnp.bfloat16),
            pltpu.VMEM(block, jnp.bfloat16),
            pltpu.VMEM((CHUNKS, 4, 4, 8, DIM), jnp.float32),
            pltpu.VMEM((4, CHUNKS, 2, 2, 2, TOK, DIM), jnp.bfloat16),
            dma((CHUNKS, 4)),
            dma((3, CHUNKS, 4)),
            dma((3, CHUNKS, 4)),
            dma((2, CHUNKS, 2, 2)),
            dma((2, CHUNKS, 2, 2)),
            dma((2, CHUNKS, 2, 2)),
            dma((2, CHUNKS, 2, 2)),
            dma((CHUNKS, 2, 2)),
            dma((CHUNKS, 2, 2)),
            dma((CHUNKS, 2, 2)),
            dma((CHUNKS, 2, 2)),
            dma((CHUNKS, 8)),
            dma((CHUNKS, 8)),
            dma((4, CHUNKS)),
            dma((3, 4, CHUNKS)),
            dma((3, 4, CHUNKS)),
        ],
        compiler_params=pltpu.CompilerParams(
            collective_id=0, has_side_effects=True, vmem_limit_bytes=40*1024*1024
        ),
    )(*(pltpu.with_memory_space_constraint(a, pltpu.HBM) for a in (queries, keys, values, grad_out)))
    return pl.pallas_call(
        drain,
        out_shape=[jax.ShapeDtypeStruct(queries.shape, jnp.bfloat16)] * 4,
        in_specs=[pl.BlockSpec(memory_space=pl.ANY)] * 4,
        out_specs=[pl.BlockSpec(memory_space=pl.ANY)] * 4,
        scratch_shapes=[dma((4,))],
        compiler_params=pltpu.CompilerParams(vmem_limit_bytes=1024 * 1024),
    )(*held)


def solution(mesh):
    spec = P("ta", "gy", "gx", None, None)
    return jax.shard_map(
        body, mesh=mesh, in_specs=(spec,) * 4, out_specs=(spec,) * 4, check_vma=False
    )
```

```python
import jax
import jax.numpy as jnp
from jax import lax
from jax.experimental import pallas as pl
from jax.experimental.pallas import tpu as pltpu
from jax.sharding import PartitionSpec as P

MESH = pl.DeviceIdType.MESH
DIM = 128
TOK = 64
CHUNKS = 3
FACTOR = DIM ** -0.5
SCALE = FACTOR * 1.4426950408889634
FAR = 1e30
FRAMES = 16
TCOLS = 16
NT = (((1,), (1,)), ((), ()))
NN = (((1,), (0,)), ((), ()))


def dot_nt(a, b):
    return lax.dot_general(a, b, NT, preferred_element_type=jnp.float32)


def dot_nn(a, b):
    return lax.dot_general(a, b, NN, preferred_element_type=jnp.float32)


def kernel(
    q_in, k_in, v_in, g_in, out_o, out_dq, out_dk, out_dv,
    kv, qg, st, stage,
    in_send, in_recv, edge_send, y_recv, z_recv, corner_send, cy_recv, cz_recv,
    st_send, st_recv, back_send, back_recv,
):
    ta = lax.axis_index("ta")
    xl = lax.axis_index("gy")
    gx = lax.axis_index("gx")
    z, core = ta // 2, ta % 2
    xh = gx // 4
    side = (xl + xh) % 2

    def along_y(step):
        other = (gx + step + 8) % 8
        return (ta, (side + other // 4) % 2, other)

    def along_z(step):
        return (((z + step + 8) % 8) * 2 + core, xl, gx)

    peers = ((0, 1), (1, 0), (1, 1))

    def peer_id(p):
        dx, dc = peers[p]
        return (z * 2 + (core + dc) % 2, (xl + dx) % 2, gx)

    def peer_group(p):
        dx, dc = peers[p]
        return 2 * ((side + dx) % 2) + (core + dc) % 2

    my_group = 2 * side + core
    around = ((1, 0), (-1, 0), (0, 1), (0, -1), (1, 1), (1, -1), (-1, 1), (-1, -1))
    around_ids = tuple((along_z(dz)[0], *along_y(dy)[1:]) for dy, dz in around)
    y_ids, z_ids = around_ids[:2], around_ids[2:4]

    barrier = pltpu.get_barrier_semaphore()
    for target in (peer_id(0), peer_id(1), peer_id(2), *around_ids):
        pl.semaphore_signal(barrier, inc=1, device_id=target, device_id_type=MESH)
    pl.semaphore_wait(barrier, 11)

    def lanes(group, j):
        return pl.ds(pl.multiple_of((group * CHUNKS + j) * DIM, DIM), DIM)

    sources = (k_in, v_in, q_in, g_in)
    results = (out_o, out_dq, out_dk, out_dv)

    def slot(t, j):
        held = kv if t < 2 else qg
        return held.at[j, t % 2, pl.ds(1, 2), 1 + core, xl]

    def local_copy(j, t):
        return pltpu.make_async_copy(
            sources[t].at[0, 0, :, :, lanes(my_group, j)], slot(t, j), in_recv.at[j, 0, t // 2]
        )

    def in_copy(p, j, t):
        return pltpu.make_async_remote_copy(
            src_ref=sources[t].at[0, 0, :, :, lanes(peer_group(p), j)],
            dst_ref=slot(t, j),
            send_sem=in_send,
            recv_sem=in_recv.at[j, min(p, 1), t // 2],
            device_id=peer_id(p),
            device_id_type=MESH,
        )

    def remote(src, dst, send, recv, target):
        return pltpu.make_async_remote_copy(
            src_ref=src, dst_ref=dst, send_sem=send, recv_sem=recv,
            device_id=target, device_id_type=MESH,
        )

    def edge_y(h, j, w, d):
        row = (xl + w) % 2
        held = (kv, qg)[h]
        return remote(
            held.at[j, :, 2 - d, pl.ds(1, 2), row], held.at[j, :, 3 * d, pl.ds(1, 2), row],
            edge_send, y_recv.at[h, j], y_ids[d],
        )

    def edge_z(h, j, w, d):
        row = (xl + w) % 2
        held = (kv, qg)[h]
        return remote(
            held.at[j, :, pl.ds(1, 2), 2 - d, row], held.at[j, :, pl.ds(1, 2), 3 * d, row],
            edge_send, z_recv.at[h, j], z_ids[d],
        )

    def corner_z(j, e, d):
        return remote(
            kv.at[j, :, 3 * e, 2 - d], kv.at[j, :, 3 * e, 3 * d],
            corner_send, cz_recv.at[j], z_ids[d],
        )

    def corner_y(j, e, d):
        return remote(
            qg.at[j, :, 2 - d, 3 * e], qg.at[j, :, 3 * d, 3 * e],
            corner_send, cy_recv.at[j], y_ids[d],
        )

    def stat_copy(j, n):
        dy, dz = around[n]
        cols = {0: (pl.ds(1, 2), pl.ds(1, 2)), 1: (2, 0), -1: (1, 3)}[dy]
        frames = {0: (pl.ds(1, 2), pl.ds(1, 2)), 1: (2, 0), -1: (1, 3)}[dz]
        return remote(
            st.at[j, cols[0], frames[0]], st.at[j, cols[1], frames[1]],
            st_send, st_recv.at[j], around_ids[n],
        )

    def keep_copy(t, j):
        return pltpu.make_async_copy(
            stage.at[t, j, :, core, xl], results[t].at[0, 0, :, :, lanes(my_group, j)],
            back_recv,
        )

    def back_copy(p, t, j):
        dx, dc = peers[p]
        return remote(
            stage.at[t, j, :, (core + dc) % 2, (xl + dx) % 2],
            results[t].at[0, 0, :, :, lanes(my_group, j)],
            back_send, back_recv, peer_id(p),
        )

    for j in range(CHUNKS):
        for t in range(4):
            local_copy(j, t).start()
            in_copy(0, j, t).start()
    for j in range(CHUNKS):
        for t in range(4):
            for p in (1, 2):
                in_copy(p, j, t).start()

    def settle(sem, like):
        pltpu.make_async_copy(like, like, sem).wait()

    def first_hops(j, w):
        row = (xl + w) % 2
        for h in range(2):
            settle(in_recv.at[j, w, h], (kv, qg)[h].at[j, :, pl.ds(1, 2), pl.ds(1, 2), row])
            for d in range(2):
                edge_y(h, j, w, d).start()
                edge_z(h, j, w, d).start()

    def second_hops(j):
        settle(y_recv.at[0, j], kv.at[j, :, pl.ds(0, 2), pl.ds(1, 2)])
        for e in range(2):
            for d in range(2):
                corner_z(j, e, d).start()
        settle(z_recv.at[1, j], qg.at[j, :, pl.ds(1, 2), pl.ds(0, 2)])
        for e in range(2):
            for d in range(2):
                corner_y(j, e, d).start()

    def in_grid(c, f, dc, df):
        col = 2 * gx + c + dc - 1
        frame = 2 * z + f + df - 1
        return (col >= 0) & (col < TCOLS) & (frame >= 0) & (frame < FRAMES)

    lane = lax.broadcasted_iota(jnp.int32, (DIM, DIM), 1)

    def pair(half0, half1):
        blank = jnp.zeros((2 * TOK, DIM), half0.dtype)
        return jnp.concatenate(
            [jnp.concatenate([half0, blank], axis=1), jnp.concatenate([blank, half1], axis=1)],
            axis=0,
        )

    def halves(x):
        return x[:2 * TOK, :3 * DIM], x[2 * TOK:, DIM:]

    def query_block(j, c):
        q = qg[j, 0, 1 + c, 1:3].reshape(4 * TOK, DIM)
        g = qg[j, 1, 1 + c, 1:3].reshape(4 * TOK, DIM)
        scores = [[], []]
        for dc in range(3):
            s = dot_nt(q, kv[j, 0, c + dc].reshape(8 * TOK, DIM))
            for f, part in enumerate(halves(s)):
                scores[f].append(jnp.concatenate([
                    part[:, df * DIM:(df + 1) * DIM] * SCALE
                    + jnp.where(in_grid(c, f, dc, df), 0.0, -FAR)
                    for df in range(3)
                ], axis=1))
        tops, powers, totals = [], [], []
        for f in range(2):
            top = jnp.maximum(jnp.maximum(scores[f][0], scores[f][1]), scores[f][2])
            top = jnp.max(top, axis=1, keepdims=True)
            p = [jnp.exp2(s - top) for s in scores[f]]
            tops.append(top)
            powers.append(p)
            totals.append(jnp.sum(p[0] + p[1] + p[2], axis=1, keepdims=True))
        top = jnp.concatenate(tops, axis=0)
        total = jnp.concatenate(totals, axis=0)
        scale = 1.0 / total
        att = jnp.zeros((4 * TOK, DIM), jnp.float32)
        for dc in range(3):
            v = kv[j, 1, c + dc].reshape(8 * TOK, DIM)
            att += dot_nn(pair(*(powers[f][dc].astype(jnp.bfloat16) for f in range(2))), v)
        att = (att * scale).astype(jnp.bfloat16)
        dots = jnp.sum(g.astype(jnp.float32) * att.astype(jnp.float32), axis=1, keepdims=True)
        grad = jnp.zeros((4 * TOK, DIM), jnp.float32)
        for dc in range(3):
            k = kv[j, 0, c + dc].reshape(8 * TOK, DIM)
            v = kv[j, 1, c + dc].reshape(8 * TOK, DIM)
            pulls = halves(dot_nt(g, v))
            slopes = (
                (powers[f][dc] * (pulls[f] - dots[f * 2 * TOK:(f + 1) * 2 * TOK])).astype(jnp.bfloat16)
                for f in range(2)
            )
            grad += dot_nn(pair(*slopes), k)
        grad = (grad * (scale * FACTOR)).astype(jnp.bfloat16)
        stage[0, j, c] = att.reshape(2, 2, TOK, DIM)
        stage[1, j, c] = grad.reshape(2, 2, TOK, DIM)
        level = top + jnp.log2(total)
        for f in range(2):
            cut = slice(f * 2 * TOK, (f + 1) * 2 * TOK)
            st[j, 1 + c, 1 + f] = jnp.transpose(jnp.where(lane == 0, level[cut], dots[cut]))[:8]

    def key_block(j, c):
        k = kv[j, 0, 1 + c, 1:3].reshape(4 * TOK, DIM)
        v = kv[j, 1, 1 + c, 1:3].reshape(4 * TOK, DIM)
        grad_k = jnp.zeros((4 * TOK, DIM), jnp.float32)
        grad_v = jnp.zeros((4 * TOK, DIM), jnp.float32)
        for dc in range(3):
            q = qg[j, 0, c + dc].reshape(8 * TOK, DIM)
            g = qg[j, 1, c + dc].reshape(8 * TOK, DIM)
            s = halves(dot_nt(k, q))
            pulls = halves(dot_nt(v, g))
            weights, slopes = [], []
            for f in range(2):
                ws, ss = [], []
                for df in range(3):
                    tile = st[j, c + dc, f + df]
                    level = jnp.where(in_grid(c, f, dc, df), tile[0:1], FAR)
                    cut = slice(df * DIM, (df + 1) * DIM)
                    w = jnp.exp2(s[f][:, cut] * SCALE - level)
                    ws.append(w.astype(jnp.bfloat16))
                    ss.append((w * (pulls[f][:, cut] - tile[1:2])).astype(jnp.bfloat16))
                weights.append(jnp.concatenate(ws, axis=1))
                slopes.append(jnp.concatenate(ss, axis=1))
            grad_v += dot_nn(pair(*weights), g)
            grad_k += dot_nn(pair(*slopes), q)
        stage[2, j, c] = (grad_k * FACTOR).astype(jnp.bfloat16).reshape(2, 2, TOK, DIM)
        stage[3, j, c] = grad_v.astype(jnp.bfloat16).reshape(2, 2, TOK, DIM)

    def blocks(run, j):
        def one(c, carry):
            run(j, c)
            return carry

        lax.fori_loop(0, 2, one, 0)

    def send_back(j, ts):
        for t in ts:
            for p in (1, 2, 0):
                back_copy(p, t, j).start()
            keep_copy(t, j).start()

    def query_side(j):
        settle(z_recv.at[0, j], kv.at[j, :, pl.ds(1, 2), pl.ds(0, 2)])
        settle(cz_recv.at[j], kv.at[j, :, pl.ds(0, 2), pl.ds(0, 2)])
        blocks(query_block, j)
        for n in range(8):
            stat_copy(j, n).start()
        send_back(j, (0, 1))

    def key_side(j):
        settle(y_recv.at[1, j], qg.at[j, :, pl.ds(0, 2), pl.ds(1, 2)])
        settle(cy_recv.at[j], qg.at[j, :, pl.ds(0, 2), pl.ds(0, 2)])
        settle(st_recv.at[j], st.at[j, pl.ds(0, 3)])
        blocks(key_block, j)
        send_back(j, (2, 3))

    first_hops(0, 0)
    first_hops(1, 0)
    first_hops(0, 1)
    first_hops(2, 0)
    second_hops(0)
    first_hops(1, 1)
    first_hops(2, 1)
    second_hops(1)
    query_side(0)
    second_hops(2)
    query_side(1)
    key_side(0)
    query_side(2)
    key_side(1)
    key_side(2)
    settle(in_send, kv.at[:, :, pl.ds(0, 3), :, 0])
    settle(edge_send, kv)
    settle(corner_send, kv.at[:, :, pl.ds(0, 2)])
    settle(st_send, st.at[:, pl.ds(0, 3)])
    settle(back_send, kv.at[:, :, pl.ds(0, 3), :, 0])
    settle(back_recv, kv.at[:, :, pl.ds(0, 2)])


def drain(*refs):
    held, out, sem = refs[:4], refs[4:8], refs[8]
    copies = [pltpu.make_async_copy(held[t], out[t], sem.at[t]) for t in range(4)]
    for copy in copies:
        copy.start()
    for copy in copies:
        copy.wait()


def body(queries, keys, values, grad_out):
    dma = pltpu.SemaphoreType.DMA
    block = (CHUNKS, 2, 4, 4, 2, TOK, DIM)
    held = pl.pallas_call(
        kernel,
        out_shape=[jax.ShapeDtypeStruct(queries.shape, jnp.bfloat16)] * 4,
        in_specs=[pl.BlockSpec(memory_space=pl.ANY)] * 4,
        out_specs=[pl.BlockSpec(memory_space=pl.ANY)] * 4,
        scratch_shapes=[
            pltpu.VMEM(block, jnp.bfloat16),
            pltpu.VMEM(block, jnp.bfloat16),
            pltpu.VMEM((CHUNKS, 4, 4, 8, DIM), jnp.float32),
            pltpu.VMEM((4, CHUNKS, 2, 2, 2, TOK, DIM), jnp.bfloat16),
            dma(()),
            dma((CHUNKS, 2, 2)),
            dma(()),
            dma((2, CHUNKS)),
            dma((2, CHUNKS)),
            dma(()),
            dma((CHUNKS,)),
            dma((CHUNKS,)),
            dma(()),
            dma((CHUNKS,)),
            dma(()),
            dma(()),
        ],
        compiler_params=pltpu.CompilerParams(
            collective_id=0, has_side_effects=True, vmem_limit_bytes=40*1024*1024
        ),
    )(*(pltpu.with_memory_space_constraint(a, pltpu.HBM) for a in (queries, keys, values, grad_out)))
    return pl.pallas_call(
        drain,
        out_shape=[jax.ShapeDtypeStruct(queries.shape, jnp.bfloat16)] * 4,
        in_specs=[pl.BlockSpec(memory_space=pl.ANY)] * 4,
        out_specs=[pl.BlockSpec(memory_space=pl.ANY)] * 4,
        scratch_shapes=[dma((4,))],
        compiler_params=pltpu.CompilerParams(vmem_limit_bytes=1024 * 1024),
    )(*held)


def solution(mesh):
    spec = P("ta", "gy", "gx", None, None)
    return jax.shard_map(
        body, mesh=mesh, in_specs=(spec,) * 4, out_specs=(spec,) * 4, check_vma=False
    )
```

```python
import functools

import jax
import jax.numpy as jnp
from jax import lax
from jax.experimental import pallas as pl
from jax.experimental.pallas import tpu as pltpu
from jax.sharding import PartitionSpec as P

MESH = pl.DeviceIdType.MESH
DIM = 128
TOK = 64
CHUNKS = 3
FACTOR = DIM ** -0.5
SCALE = FACTOR * 1.4426950408889634
FAR = 1e30
FRAMES = 16
TCOLS = 16
NT = (((1,), (1,)), ((), ()))
NN = (((1,), (0,)), ((), ()))


def dot_nt(a, b):
    return lax.dot_general(a, b, NT, preferred_element_type=jnp.float32)


def dot_nn(a, b):
    return lax.dot_general(a, b, NN, preferred_element_type=jnp.float32)


def kernel(
    q_in, k_in, v_in, g_in, out_o, out_dq, out_dk, out_dv,
    kv, qg, st, stage,
    in_send, in_recv, edge_send, y_recv, z_recv, corner_send, cy_recv, cz_recv,
    st_send, st_recv, back_send, back_recv,
):
    ta = lax.axis_index("ta")
    xl = lax.axis_index("gy")
    gx = lax.axis_index("gx")
    z, core = ta // 2, ta % 2
    xh = gx // 4
    side = (xl + xh) % 2

    def along_y(step):
        other = (gx + step + 8) % 8
        return (ta, (side + other // 4) % 2, other)

    def along_z(step):
        return (((z + step + 8) % 8) * 2 + core, xl, gx)

    peers = ((0, 1), (1, 0), (1, 1))

    def peer_id(p):
        dx, dc = peers[p]
        return (z * 2 + (core + dc) % 2, (xl + dx) % 2, gx)

    def peer_group(p):
        dx, dc = peers[p]
        return 2 * ((side + dx) % 2) + (core + dc) % 2

    my_group = 2 * side + core
    around = ((1, 0), (-1, 0), (0, 1), (0, -1), (1, 1), (1, -1), (-1, 1), (-1, -1))
    around_ids = tuple((along_z(dz)[0], *along_y(dy)[1:]) for dy, dz in around)
    y_ids, z_ids = around_ids[:2], around_ids[2:4]

    barrier = pltpu.get_barrier_semaphore()
    for target in (peer_id(0), peer_id(1), peer_id(2), *around_ids):
        pl.semaphore_signal(barrier, inc=1, device_id=target, device_id_type=MESH)
    pl.semaphore_wait(barrier, 11)

    def lanes(group, j):
        return pl.ds(pl.multiple_of((group * CHUNKS + j) * DIM, DIM), DIM)

    sources = (k_in, v_in, q_in, g_in)
    results = (out_o, out_dq, out_dk, out_dv)

    def slot(t, j):
        held = kv if t < 2 else qg
        return held.at[j, t % 2, pl.ds(1, 2), 1 + core, xl]

    def local_copy(j, t):
        return pltpu.make_async_copy(
            sources[t].at[0, 0, :, :, lanes(my_group, j)], slot(t, j), in_recv.at[j, 0, t // 2]
        )

    def in_copy(p, j, t):
        return pltpu.make_async_remote_copy(
            src_ref=sources[t].at[0, 0, :, :, lanes(peer_group(p), j)],
            dst_ref=slot(t, j),
            send_sem=in_send,
            recv_sem=in_recv.at[j, min(p, 1), t // 2],
            device_id=peer_id(p),
            device_id_type=MESH,
        )

    def remote(src, dst, send, recv, target):
        return pltpu.make_async_remote_copy(
            src_ref=src, dst_ref=dst, send_sem=send, recv_sem=recv,
            device_id=target, device_id_type=MESH,
        )

    def edge_y(h, j, w, d):
        row = (xl + w) % 2
        held = (kv, qg)[h]
        return remote(
            held.at[j, :, 2 - d, pl.ds(1, 2), row], held.at[j, :, 3 * d, pl.ds(1, 2), row],
            edge_send, y_recv.at[h, j], y_ids[d],
        )

    def edge_z(h, j, w, d):
        row = (xl + w) % 2
        held = (kv, qg)[h]
        return remote(
            held.at[j, :, pl.ds(1, 2), 2 - d, row], held.at[j, :, pl.ds(1, 2), 3 * d, row],
            edge_send, z_recv.at[h, j], z_ids[d],
        )

    def corner_z(j, e, d):
        return remote(
            kv.at[j, :, 3 * e, 2 - d], kv.at[j, :, 3 * e, 3 * d],
            corner_send, cz_recv.at[j], z_ids[d],
        )

    def corner_y(j, e, d):
        return remote(
            qg.at[j, :, 2 - d, 3 * e], qg.at[j, :, 3 * d, 3 * e],
            corner_send, cy_recv.at[j], y_ids[d],
        )

    def stat_copy(j, n):
        dy, dz = around[n]
        cols = {0: (pl.ds(1, 2), pl.ds(1, 2)), 1: (2, 0), -1: (1, 3)}[dy]
        frames = {0: (pl.ds(1, 2), pl.ds(1, 2)), 1: (2, 0), -1: (1, 3)}[dz]
        return remote(
            st.at[j, cols[0], frames[0]], st.at[j, cols[1], frames[1]],
            st_send, st_recv.at[j], around_ids[n],
        )

    def keep_copy(t, j, c):
        return pltpu.make_async_copy(
            stage.at[t, j, c, core, xl], results[t].at[0, 0, c, :, lanes(my_group, j)],
            back_recv,
        )

    def back_copy(p, t, j, c):
        dx, dc = peers[p]
        return remote(
            stage.at[t, j, c, (core + dc) % 2, (xl + dx) % 2],
            results[t].at[0, 0, c, :, lanes(my_group, j)],
            back_send, back_recv, peer_id(p),
        )

    for j in range(CHUNKS):
        for t in range(4):
            local_copy(j, t).start()
            in_copy(0, j, t).start()
    for j in range(CHUNKS):
        for t in range(4):
            for p in (1, 2):
                in_copy(p, j, t).start()

    def settle(sem, like):
        pltpu.make_async_copy(like, like, sem).wait()

    def first_hops(j, w):
        row = (xl + w) % 2
        for h in range(2):
            settle(in_recv.at[j, w, h], (kv, qg)[h].at[j, :, pl.ds(1, 2), pl.ds(1, 2), row])
            for d in range(2):
                edge_y(h, j, w, d).start()
                edge_z(h, j, w, d).start()

    def second_hops(j):
        settle(y_recv.at[0, j], kv.at[j, :, pl.ds(0, 2), pl.ds(1, 2)])
        for e in range(2):
            for d in range(2):
                corner_z(j, e, d).start()
        settle(z_recv.at[1, j], qg.at[j, :, pl.ds(1, 2), pl.ds(0, 2)])
        for e in range(2):
            for d in range(2):
                corner_y(j, e, d).start()

    def in_grid(ci, fi):
        col = 2 * gx + ci - 1
        frame = 2 * z + fi - 1
        return (col >= 0) & (col < TCOLS) & (frame >= 0) & (frame < FRAMES)

    lane = lax.broadcasted_iota(jnp.int32, (DIM, DIM), 1)

    own = (slice(0, 2 * TOK), slice(2 * TOK, 4 * TOK))

    def inner(held, j, t, c):
        return held[j, t, pl.ds(c, 3), 1:3].reshape(12 * TOK, DIM)

    def outer(held, j, t, c, f):
        return held[j, t, pl.ds(c, 3), 3 * f].reshape(6 * TOK, DIM)

    def by_rows(make):
        return jnp.concatenate([make(0), make(1)], axis=0)

    def cuts(x):
        return [x[:, n * DIM:(n + 1) * DIM] for n in range(x.shape[1] // DIM)]

    def times(left, right, held, j, t, c):
        return dot_nn(left, inner(held, j, t, c)) + by_rows(
            lambda f: dot_nn(right[own[f]], outer(held, j, t, c, f))
        )

    def against(rows, held, j, t, c):
        near = cuts(dot_nt(rows, inner(held, j, t, c)))
        far = cuts(by_rows(lambda f: dot_nt(rows[own[f]], outer(held, j, t, c, f))))
        return near + far

    def query_block(j, c):
        q = qg[j, 0, 1 + c, 1:3].reshape(4 * TOK, DIM)
        g = qg[j, 1, 1 + c, 1:3].reshape(4 * TOK, DIM)
        bias = lambda ci, fi: jnp.where(in_grid(ci, fi), 0.0, -FAR)
        scores = against(q, kv, j, 0, c)
        for n in range(6):
            scores[n] = scores[n] * SCALE + bias(c + n // 2, 1 + n % 2)
        for n in range(3):
            part = scores[6 + n] * SCALE
            scores[6 + n] = by_rows(lambda f: part[own[f]] + bias(c + n, 3 * f))
        top = functools.reduce(jnp.maximum, scores)
        top = jnp.max(top, axis=1, keepdims=True)
        powers = [jnp.exp2(s - top) for s in scores]
        total = jnp.sum(functools.reduce(jnp.add, powers), axis=1, keepdims=True)
        scale = 1.0 / total

        def rounded(parts):
            parts = [p.astype(jnp.bfloat16) for p in parts]
            return jnp.concatenate(parts[:6], axis=1), jnp.concatenate(parts[6:], axis=1)

        att = (times(*rounded(powers), kv, j, 1, c) * scale).astype(jnp.bfloat16)
        dots = jnp.sum(g.astype(jnp.float32) * att.astype(jnp.float32), axis=1, keepdims=True)
        pulls = against(g, kv, j, 1, c)
        slopes = [p * (x - dots) for p, x in zip(powers, pulls)]
        grad = times(*rounded(slopes), kv, j, 0, c)
        grad = (grad * (scale * FACTOR)).astype(jnp.bfloat16)
        stage[0, j, c] = att.reshape(2, 2, TOK, DIM)
        stage[1, j, c] = grad.reshape(2, 2, TOK, DIM)
        level = top + jnp.log2(total)
        for f in range(2):
            both = jnp.where(lane == 0, level[own[f]], dots[own[f]])
            st[j, 1 + c, 1 + f] = jnp.transpose(both)[:8]

    def key_block(j, c):
        k = kv[j, 0, 1 + c, 1:3].reshape(4 * TOK, DIM)
        v = kv[j, 1, 1 + c, 1:3].reshape(4 * TOK, DIM)

        def rows_of(ci, fi):
            tile = st[j, ci, fi]
            return jnp.where(in_grid(ci, fi), tile[0:1], FAR), tile[1:2]

        def weigh(s, x, ci, fi):
            level, dots = rows_of(ci, fi)
            w = jnp.exp2(s * SCALE - level)
            return w.astype(jnp.bfloat16), (w * (x - dots)).astype(jnp.bfloat16)

        scores = against(k, qg, j, 0, c)
        pulls = against(v, qg, j, 1, c)
        near = [weigh(scores[n], pulls[n], c + n // 2, 1 + n % 2) for n in range(6)]
        far = [
            [weigh(scores[6 + n][own[f]], pulls[6 + n][own[f]], c + n, 3 * f) for n in range(3)]
            for f in range(2)
        ]
        grads = []
        for i, t in ((0, 1), (1, 0)):
            left = jnp.concatenate([x[i] for x in near], axis=1)
            right = by_rows(lambda f: jnp.concatenate([x[i] for x in far[f]], axis=1))
            grads.append(times(left, right, qg, j, t, c))
        stage[2, j, c] = (grads[1] * FACTOR).astype(jnp.bfloat16).reshape(2, 2, TOK, DIM)
        stage[3, j, c] = grads[0].astype(jnp.bfloat16).reshape(2, 2, TOK, DIM)

    def blocks(run, j, ts):
        def one(c, carry):
            run(j, c)
            send_back(j, c, ts)
            return carry

        lax.fori_loop(0, 2, one, 0)

    def send_back(j, c, ts):
        for t in ts:
            for p in (1, 2, 0):
                back_copy(p, t, j, c).start()
            keep_copy(t, j, c).start()

    def query_side(j):
        settle(z_recv.at[0, j], kv.at[j, :, pl.ds(1, 2), pl.ds(0, 2)])
        settle(cz_recv.at[j], kv.at[j, :, pl.ds(0, 2), pl.ds(0, 2)])
        blocks(query_block, j, (0, 1))
        for n in range(8):
            stat_copy(j, n).start()

    def key_side(j):
        settle(y_recv.at[1, j], qg.at[j, :, pl.ds(0, 2), pl.ds(1, 2)])
        settle(cy_recv.at[j], qg.at[j, :, pl.ds(0, 2), pl.ds(0, 2)])
        settle(st_recv.at[j], st.at[j, pl.ds(0, 3)])
        blocks(key_block, j, (2, 3))

    first_hops(0, 0)
    first_hops(1, 0)
    first_hops(0, 1)
    first_hops(2, 0)
    second_hops(0)
    first_hops(1, 1)
    first_hops(2, 1)
    second_hops(1)
    query_side(0)
    second_hops(2)
    query_side(1)
    key_side(0)
    query_side(2)
    key_side(1)
    key_side(2)
    settle(in_send, kv.at[:, :, pl.ds(0, 3), :, 0])
    settle(edge_send, kv)
    settle(corner_send, kv.at[:, :, pl.ds(0, 2)])
    settle(st_send, st.at[:, pl.ds(0, 3)])
    settle(back_send, kv.at[:, :, pl.ds(0, 3), :, 0])
    settle(back_recv, kv.at[:, :, pl.ds(0, 2)])


def drain(*refs):
    held, out, sem = refs[:4], refs[4:8], refs[8]
    copies = [pltpu.make_async_copy(held[t], out[t], sem.at[t]) for t in range(4)]
    for copy in copies:
        copy.start()
    for copy in copies:
        copy.wait()


def body(queries, keys, values, grad_out):
    dma = pltpu.SemaphoreType.DMA
    block = (CHUNKS, 2, 4, 4, 2, TOK, DIM)
    held = pl.pallas_call(
        kernel,
        out_shape=[jax.ShapeDtypeStruct(queries.shape, jnp.bfloat16)] * 4,
        in_specs=[pl.BlockSpec(memory_space=pl.ANY)] * 4,
        out_specs=[pl.BlockSpec(memory_space=pl.ANY)] * 4,
        scratch_shapes=[
            pltpu.VMEM(block, jnp.bfloat16),
            pltpu.VMEM(block, jnp.bfloat16),
            pltpu.VMEM((CHUNKS, 4, 4, 8, DIM), jnp.float32),
            pltpu.VMEM((4, CHUNKS, 2, 2, 2, TOK, DIM), jnp.bfloat16),
            dma(()),
            dma((CHUNKS, 2, 2)),
            dma(()),
            dma((2, CHUNKS)),
            dma((2, CHUNKS)),
            dma(()),
            dma((CHUNKS,)),
            dma((CHUNKS,)),
            dma(()),
            dma((CHUNKS,)),
            dma(()),
            dma(()),
        ],
        compiler_params=pltpu.CompilerParams(
            collective_id=0, has_side_effects=True, vmem_limit_bytes=40*1024*1024
        ),
    )(*(pltpu.with_memory_space_constraint(a, pltpu.HBM) for a in (queries, keys, values, grad_out)))
    return pl.pallas_call(
        drain,
        out_shape=[jax.ShapeDtypeStruct(queries.shape, jnp.bfloat16)] * 4,
        in_specs=[pl.BlockSpec(memory_space=pl.ANY)] * 4,
        out_specs=[pl.BlockSpec(memory_space=pl.ANY)] * 4,
        scratch_shapes=[dma((4,))],
        compiler_params=pltpu.CompilerParams(vmem_limit_bytes=1024 * 1024),
    )(*held)


def solution(mesh):
    spec = P("ta", "gy", "gx", None, None)
    return jax.shard_map(
        body, mesh=mesh, in_specs=(spec,) * 4, out_specs=(spec,) * 4, check_vma=False
    )
```
